32 devices in a mesh: dp: 4 (over x, y), sp: 8 (over z, core).
Axes of the slice: x: 2, y: 2, z: 4, core: 2. Of those that a mesh axis runs over, the one named last changes fastest.
Arguments:
- q: bfloat16 [128, 96, 192], P('dp'), parts along dimension 0
- k: bfloat16 [128, 4096, 8, 192], P('dp', 'sp'), parts along dimension 0
- v: bfloat16 [128, 4096, 8, 192], P('dp', 'sp'), parts along dimension 0
Outputs:
- q: bfloat16 [128, 96, 192], P('dp'), parts along dimension 0
There are 4 independent parts. The reference program is written for one: setup_inputs(seed, part) draws one part's arguments, and reference() takes and returns one part's arrays. A program takes and returns all parts, laid end to end along the dimension named above; each array names one.
All inputs are finite; a program needn't handle non-finite values.
Results may differ from the reference program's by a relative error of at most 0.012.
Values are sent between devices in bfloat16 or wider.
A program may use at most 2 GiB of HBM per device.

```python
import jax
import jax.numpy as jnp

BATCH = 32
CACHE = 4096
HEADS = 96
KV_HEADS = 8
HEAD = 192


def setup_inputs(seed: int = 0, part: int = 0) -> dict:
    kq, kk, kv = (jax.random.fold_in(k, part) for k in jax.random.split(jax.random.key(seed), 3))
    return {
        "q": (3 * jax.random.normal(kq, (BATCH, HEADS, HEAD), jnp.float32)).astype(jnp.bfloat16),
        "k": jax.random.normal(kk, (BATCH, CACHE, KV_HEADS, HEAD), jnp.float32).astype(jnp.bfloat16),
        "v": jax.random.normal(kv, (BATCH, CACHE, KV_HEADS, HEAD), jnp.float32).astype(jnp.bfloat16),
    }


def einsum(form, a, b):
    return jnp.einsum(form, a.astype(jnp.float32), b.astype(jnp.float32))


def reference(q, k, v):
    grouped = q.reshape(BATCH, KV_HEADS, -1, HEAD)
    scores = einsum("bgsd,bugd->bgsu", grouped, k) * HEAD**-0.5
    weights = jax.nn.softmax(scores, -1).astype(jnp.bfloat16)
    return einsum("bgsu,bugd->bgsd", weights, v).astype(jnp.bfloat16).reshape(BATCH, HEADS, HEAD)
```

```python
import functools
import math

import jax
import jax.numpy as jnp
from jax import lax
from jax.experimental import pallas as pl
from jax.experimental.pallas import tpu as pltpu
from jax.sharding import PartitionSpec as P

F32, BF16 = jnp.float32, jnp.bfloat16
HEAD = 192
SHARE = 12
ROWS = 4 * SHARE
WIDE = 4 * HEAD
RATE = HEAD**-0.5 * math.log2(math.e)
PACK = 72
BATCH = 4
LEAD = 12
DEPTH = 6
HOP = dict(chip=2, outer=7, middle=12, last=17, out=20)
MESH = pl.DeviceIdType.MESH


def lanes(shape):
    return lax.broadcasted_iota(jnp.int32, shape, 1)


def rows(shape):
    return lax.broadcasted_iota(jnp.int32, shape, 0)


def spread(q):
    q = jnp.concatenate([q.astype(F32), jnp.zeros((ROWS, 256 - HEAD), F32)], 1)
    a, b = q[:, :128], q[:, 128:]
    ra, rb = pltpu.roll(a, 64, 1), pltpu.roll(b, 64, 1)
    low, head = lanes(a.shape) < 64, rows(a.shape) // SHARE
    x1, x2 = jnp.where(low, b, ra), jnp.where(low, ra, rb)
    tiles = []
    for first in (0, 2):
        tiles.append(jnp.where(head == first, a, 0.0))
        tiles.append(jnp.where(head == jnp.where(low, first, first + 1), x1, 0.0))
        tiles.append(jnp.where(head == first + 1, x2, 0.0))
    return jnp.concatenate(tiles, 1).astype(BF16)


def fold(o):
    t = [o[:, 128 * i : 128 * (i + 1)] for i in range(6)]
    low, head = lanes(t[0].shape) < 64, rows(t[0].shape) // SHARE
    lo = jnp.where(
        head == 0,
        t[0],
        jnp.where(
            head == 1,
            pltpu.roll(jnp.where(low, t[2], t[1]), 64, 1),
            jnp.where(head == 2, t[3], pltpu.roll(jnp.where(low, t[5], t[4]), 64, 1)),
        ),
    )
    half = ROWS // 2
    upper = jnp.where(head[:half] == 0, t[1][:half], pltpu.roll(t[2][:half], 64, 1))
    lower = jnp.where(head[half:] == 2, pltpu.roll(t[4][half:], 64, 1), t[5][half:])
    return lo, jnp.where(low[:half], upper, lower)


def kernel(
    seqs, q_hbm, k_hbm, v_hbm, out, q, kbuf, vbuf, weights, column, factor, stats, give, own, got, hop_out, hop_in, mid_out, mid_in, fin, q_sem, k_sem, v_sem,
    stats_send, stats_recv, pair_send, pair_recv, hop_send, hop_recv, mid_send, mid_recv, fin_send, fin_recv,
):
    dp, me = lax.axis_index("dp"), lax.axis_index("sp")
    z, core = me // 2, me % 2
    inner = (z == 1) | (z == 2)
    partner = (dp, z * 2 + (1 - core))
    across = (dp, (3 - z) * 2 + core)
    along = (dp, (z + jnp.where(z % 2 == 0, 1, -1)) * 2 + core)

    def k_copy(s):
        return pltpu.make_async_copy(k_hbm.at[s], kbuf.at[s % DEPTH], k_sem.at[s % DEPTH])

    def v_copy(s):
        return pltpu.make_async_copy(v_hbm.at[s], vbuf.at[s % DEPTH], v_sem.at[s % DEPTH])

    q_copy = pltpu.make_async_copy(q_hbm, q, q_sem)
    q_copy.start()
    for s in range(DEPTH):
        k_copy(s).start()

    barrier = pltpu.get_barrier_semaphore()
    for step in range(1, 8):
        pl.semaphore_signal(barrier, inc=1, device_id=(dp, (me + step) % 8), device_id_type=MESH)
    for s in range(DEPTH):
        v_copy(s).start()
    column[...] = jnp.zeros_like(column)
    q_copy.wait()

    def remote(src, dst, send, recv, device):
        return pltpu.make_async_remote_copy(src_ref=src, dst_ref=dst, send_sem=send, recv_sem=recv, device_id=device, device_id_type=MESH)

    def stats_copy(b, step):
        return remote(stats.at[b, me], stats.at[b, me], stats_send.at[b, step - 1], stats_recv.at[b], (dp, (me + step) % 8))

    def pair_copy(s):
        return remote(give.at[s], got.at[s], pair_send.at[s], pair_recv.at[s], partner)

    def hop_copy(s):
        return remote(hop_out.at[s], hop_in.at[s], hop_send.at[s], hop_recv.at[s], along)

    def mid_copy(s):
        return remote(mid_out.at[s], mid_in.at[s], mid_send.at[s], mid_recv.at[s], across)

    def back_copy(s):
        return remote(fin.at[s, core], fin.at[s, core], hop_send.at[s], hop_recv.at[s], along)

    def fin_copy(s):
        return remote(fin.at[s, core], fin.at[s, core], fin_send.at[s], fin_recv.at[s], partner)

    def score(s):
        k = kbuf.at[s % DEPTH]
        j = s % BATCH
        for half in range(2):
            part = pl.ds(ROWS * half, ROWS)
            scores = jnp.dot(spread(q[s, part, :]), k[pl.ds(WIDE * half, WIDE), :], preferred_element_type=F32)
            high = jnp.max(scores, 1, keepdims=True)
            w = jnp.exp2((scores - high) * RATE)
            weights[s, half] = w.astype(BF16)
            total = jnp.sum(w, 1, keepdims=True)
            lane = lanes((ROWS, 128))
            column[part, :] = jnp.where(lane == j, high, jnp.where(lane == BATCH + j, total, column[part, :]))

    def tell(s):
        @pl.when(s % BATCH == BATCH - 1)
        def _():
            b = s // BATCH
            stats[b, me] = column[...].T[:8]
            for step in range(1, 8):
                stats_copy(b, step).start()

    def learn(s):
        @pl.when(s % BATCH == 0)
        def _():
            b = s // BATCH
            pltpu.make_async_copy(stats.at[b, pl.ds(0, 7)], stats.at[b, pl.ds(0, 7)], stats_recv.at[b]).wait()
            high = functools.reduce(jnp.maximum, [stats[b, d] for d in range(8)])
            total = sum(pltpu.roll(stats[b, d], BATCH, 0) * jnp.exp2((stats[b, d] - high) * RATE) for d in range(8))
            f = jnp.exp2((stats[b, me] - high) * RATE) / total
            factor[...] = jnp.concatenate([f] * 16, 0).T

    def gather(s):
        v = vbuf.at[s % DEPTH]
        lane = lanes((ROWS, 128))
        parts = []
        for half in range(2):
            o = lax.dot_general(weights[s, half], v[pl.ds(WIDE * half, WIDE), :], (((1,), (1,)), ((), ())), preferred_element_type=F32)
            f = jnp.sum(jnp.where(lane == s % BATCH, factor[pl.ds(ROWS * half, ROWS), :], 0.0), 1, keepdims=True)
            parts.append(jnp.concatenate(fold(o * f), 0))
        first = core == 0
        own[s] = jnp.where(first, parts[0], parts[1])
        give[s] = jnp.where(first, parts[1], parts[0]).astype(BF16)

    def inside(s):
        return (s >= 0) & (s < seqs)

    def chip(s):
        @pl.when(inside(s) & jnp.logical_not(inner))
        def _():
            pair_copy(s).wait_recv()
            hop_out[s] = (own[s] + got[s].astype(F32)).astype(BF16)
            hop_copy(s).start()

    def outer(s):
        @pl.when(inside(s) & inner)
        def _():
            pair_copy(s).wait_recv()
            hop_copy(s).wait_recv()
            mid_out[s] = (own[s] + got[s].astype(F32) + hop_in[s].astype(F32)).astype(BF16)
            mid_copy(s).start()

    def middle(s):
        @pl.when(inside(s) & inner)
        def _():
            mid_copy(s).wait_recv()
            fin[s, core] = (mid_out[s].astype(F32) + mid_in[s].astype(F32)).astype(BF16)
            back_copy(s).start()
            fin_copy(s).start()

    def last(s):
        @pl.when(inside(s) & jnp.logical_not(inner))
        def _():
            back_copy(s).wait_recv()
            fin_copy(s).start()

    def result(s):
        @pl.when(inside(s))
        def _():
            fin_copy(s).wait_recv()
            for half in range(2):
                x = fin[s, half].astype(F32)
                tail = jnp.concatenate([x[ROWS:], pltpu.roll(x[ROWS:], 64, 1)], 0)
                out[s, pl.ds(ROWS * half, ROWS), :] = jnp.concatenate([x[:ROWS], tail[:, : HEAD - 128]], 1).astype(BF16)
            pair_copy(s).wait_send()
            hop_copy(s).wait_send()
            fin_copy(s).wait_send()

            @pl.when(inner)
            def _():
                mid_copy(s).wait_send()

    def travel(t):
        chip(t - HOP["chip"])
        outer(t - HOP["outer"])
        middle(t - HOP["middle"])
        last(t - HOP["last"])
        result(t - HOP["out"])

    def head(s, _):
        k_copy(s).wait()
        score(s)
        k_copy(s + DEPTH).start()
        tell(s)

    def both(t, _):
        s = t + LEAD
        learn(t)
        k_copy(s).wait()
        v_copy(t).wait()
        score(s)
        gather(t)
        pair_copy(t).start()

        @pl.when(s + DEPTH < seqs)
        def _():
            k_copy(s + DEPTH).start()

        v_copy(t + DEPTH).start()
        tell(s)
        travel(t)

    def rest(t, _):
        learn(t)
        v_copy(t).wait()
        gather(t)
        pair_copy(t).start()

        @pl.when(t + DEPTH < seqs)
        def _():
            v_copy(t + DEPTH).start()

        travel(t)

    def drain(t, _):
        travel(t)

    def loop(low, high, body):
        lax.fori_loop(low, high, lambda i, carry: (body(i, None), carry)[1], 0)

    pl.semaphore_wait(barrier, 7)
    loop(0, LEAD, head)
    loop(0, seqs - LEAD, both)
    loop(seqs - LEAD, seqs, rest)
    loop(seqs, seqs + HOP["out"], drain)
    for b in range(seqs // BATCH):
        for step in range(1, 8):
            stats_copy(b, step).wait_send()


def attend(q, k, v):
    seqs, tokens = k.shape[:2]
    sem = pltpu.SemaphoreType.DMA
    part = lambda dtype: pltpu.VMEM((seqs, PACK, 128), dtype)
    flat = lambda x: jnp.transpose(x, (0, 2, 3, 1)).reshape(seqs, -1, tokens)
    return pl.pallas_call(
        functools.partial(kernel, seqs),
        out_shape=jax.ShapeDtypeStruct(q.shape, BF16),
        in_specs=[pl.BlockSpec(memory_space=pl.ANY)] * 3,
        out_specs=pl.BlockSpec(memory_space=pltpu.VMEM),
        scratch_shapes=[
            pltpu.VMEM(q.shape, BF16),
            pltpu.VMEM((DEPTH, 2 * WIDE, tokens), BF16),
            pltpu.VMEM((DEPTH, 2 * WIDE, tokens), BF16),
            pltpu.VMEM((seqs, 2, ROWS, tokens), BF16),
            pltpu.VMEM((128, 128), F32),
            pltpu.VMEM((128, 128), F32),
            pltpu.VMEM((seqs // BATCH, 8, 8, 128), F32),
            part(BF16), part(F32), part(BF16), part(BF16), part(BF16), part(BF16), part(BF16),
            pltpu.VMEM((seqs, 2, PACK, 128), BF16),
            sem, sem((DEPTH,)), sem((DEPTH,)),
            sem((seqs // BATCH, 7)), sem((seqs // BATCH,)),
            sem((seqs,)), sem((seqs,)), sem((seqs,)), sem((seqs,)), sem((seqs,)), sem((seqs,)), sem((seqs,)), sem((seqs,)),
        ],
        compiler_params=pltpu.CompilerParams(collective_id=0, has_side_effects=True, vmem_limit_bytes=60 << 20),
    )(q, flat(k), flat(v))


def solution(mesh):
    return jax.shard_map(
        attend,
        mesh=mesh,
        in_specs=(P("dp", None, None), P("dp", "sp", None, None), P("dp", "sp", None, None)),
        out_specs=P("dp", None, None),
        check_vma=False,
    )
```
